32 devices in a mesh: rep: 1 (over z), dp: 32 (over x, y, core).
Axes of the slice: x: 4, y: 4, z: 1, core: 2. Of those that a mesh axis runs over, the one named last changes fastest.
The devices are a block of a 4x4x8 slice.
Arguments:
- a: bfloat16 [32, 2, 4096, 512], P(('rep', 'dp'))
- g: bfloat16 [32, 2, 4096, 4096], P(('rep', 'dp'))
Outputs:
- output: bfloat16 [2, 512, 4096], P('rep')
All inputs are finite; a program needn't handle non-finite values.
Results may differ from the reference program's by a relative error of at most 0.012.
Values are sent between devices in bfloat16 or wider.
A program may use at most 768 MiB of HBM per device.

```python
import jax
import jax.numpy as jnp
from jax import lax

DEVICES = 32
MATRICES = 2
TOKENS = 4096
D = 512
FF = 4096


def setup_inputs(seed: int = 0, part: int = 0) -> dict:
    ka, kg, ks = (jax.random.fold_in(k, part) for k in jax.random.split(jax.random.key(seed), 3))
    size = 2.0 ** jax.random.uniform(ks, (DEVICES, MATRICES, 1, 1), jnp.float32, -1.0, 1.0)
    a = jax.random.normal(ka, (DEVICES, MATRICES, TOKENS, D), jnp.float32)
    g = size * jax.random.normal(kg, (DEVICES, MATRICES, TOKENS, FF), jnp.float32) * (DEVICES * TOKENS) ** -0.5
    return {"a": a.astype(jnp.bfloat16), "g": g.astype(jnp.bfloat16)}


def reference(a, g):
    def take(so_far, one):
        return so_far + jnp.einsum("ntd,ntf->ndf", *one, preferred_element_type=jnp.float32), None

    return lax.scan(take, jnp.zeros((MATRICES, D, FF), jnp.float32), (a, g))[0].astype(jnp.bfloat16)
```

```python
import functools
import math

import jax
import jax.numpy as jnp
from jax import lax
from jax.experimental import pallas as pl
from jax.experimental.pallas import tpu as pltpu
from jax.sharding import PartitionSpec as P

MESH = pl.DeviceIdType.MESH
F32, BF16 = jnp.float32, jnp.bfloat16
LANES = 128
COLS = 4 * LANES


def kernel(side, a_ref, g_ref, out_ref, av, gv, acc, mid, es, er, s1, r1, s2, r2, s3, r3, s4, r4, ag,
           a_sem, g_sem, o_sem, send_sem, e_r, r1_r, r2_r, r3_r, r4_r, g1_r, g2_r, g3_r, g4_r, z_r):
    chunks, rows = es.shape[0], es.shape[1]
    splits = av.shape[1]
    block, piece = rows // side, rows // side // side
    ring = acc.shape[0]

    me = lax.axis_index("dp")
    core = lax.rem(me, 2)
    y = lax.rem(lax.div(me, 2), side)
    x = lax.div(me, 2 * side)

    def device(x, y, core):
        return {"dp": (x * side + y) * 2 + core}

    def up(p, by=1):
        return lax.rem(p + by, side)

    peer = device(x, y, 1 - core)
    along = (
        (device(up(x), y, core), device(up(x, side - 1), y, core)),
        (device(x, up(y), core), device(x, up(y, side - 1), core)),
    )
    place = (x, y)

    def a_copy(m, h):
        matrix = 1 - core if m == 0 else core
        return pltpu.make_async_copy(a_ref.at[0, matrix, :, pl.ds(h * rows, rows)], av.at[m, h], a_sem.at[m, h])

    def g_copy(m, j, slot):
        matrix = 1 - core if m == 0 else core
        columns = pl.ds(pl.multiple_of(j * COLS, COLS), COLS)
        return pltpu.make_async_copy(g_ref.at[0, matrix, :, columns], gv.at[m, slot], g_sem.at[m, slot])

    for m in range(2):
        a_copy(m, 0).start()
        g_copy(m, 0, 0).start()
    for m in range(2):
        for h in range(1, splits):
            a_copy(m, h).start()

    barrier = pltpu.get_barrier_semaphore()
    partners = (peer, *along[0], *along[1])
    for partner in partners:
        pl.semaphore_signal(barrier, inc=1, device_id=partner, device_id_type=MESH)
    pl.semaphore_wait(barrier, len(partners))

    def remote(src, dst, stage, recv, to):
        return pltpu.make_async_remote_copy(
            src_ref=src, dst_ref=dst, send_sem=send_sem.at[stage], recv_sem=recv, device_id=to, device_id_type=MESH)

    def e_copy(s):
        return remote(es.at[s], er.at[s], 0, e_r.at[s], peer)

    def z_copy(s):
        return remote(ag.at[0, s], ag.at[1, s], 1, z_r.at[s], peer)

    def r_copy(stage, src, dst, sem, axis, s, part, way):
        return remote(src.at[s, part, way], dst.at[s, part, way], stage, sem.at[s, part, way], along[axis][way])

    r1_copy = functools.partial(r_copy, 2, s1, r1, r1_r)
    r2_copy = functools.partial(r_copy, 3, s2, r2, r2_r)
    r3_copy = functools.partial(r_copy, 4, s3, r3, r3_r)
    r4_copy = functools.partial(r_copy, 5, s4, r4, r4_r)

    def g_send(stage, view, sem, axis, s, part, way):
        return remote(view, view, stage, sem.at[s, part, way], along[axis][way])

    def two(part):
        return pl.ds(2 * part, 2)

    def at(p, size):
        return pl.ds(pl.multiple_of(p * size, size), size)

    def g1_copy(s, part, way):
        p, q = place[part], place[1 - part]
        return g_send(6, ag.at[0, s, two(part), at(p * side + q, piece)], g1_r, 1 - part, s, part, way)

    def g2_copy(s, part, way):
        p, q = place[part], place[1 - part]
        q = up(q, side - 1) if way == 0 else up(q)
        return g_send(7, ag.at[0, s, 2 * part + way, at(p * side + q, piece)], g2_r, 1 - part, s, part, way)

    def g3_copy(s, part, way):
        return g_send(8, ag.at[0, s, two(part), at(place[part], block)], g3_r, part, s, part, way)

    def g4_copy(s, part, way):
        p = place[part]
        p = up(p, side - 1) if way == 0 else up(p)
        return g_send(9, ag.at[0, s, 2 * part + way, at(p, block)], g4_r, part, s, part, way)

    def out_copies(m, s):
        matrix = core if m == 0 else 1 - core
        j, h = lax.div(s, splits), lax.rem(s, splits)
        for k in range(COLS // LANES):
            yield pltpu.make_async_copy(
                ag.at[m, s, k],
                out_ref.at[matrix, at(h, rows), pl.ds(pl.multiple_of(j * COLS + k * LANES, LANES), LANES)],
                o_sem)

    both = [(part, way) for part in range(2) for way in range(2)]

    def lane(part, half):
        return slice((2 * part + half) * LANES, (2 * part + half + 1) * LANES)

    def start_r1(s):
        c = lax.rem(s, ring)
        for part in range(2):
            p = place[part]

            def take(q, half):
                return acc[c, at(q, block), lane(part, half)].astype(BF16)

            s1[s, part, 0, 0] = take(up(p, 2), 0)
            s1[s, part, 0, 1] = take(up(p), 1)
            s1[s, part, 1, 0] = take(up(p, 2), 1)
            s1[s, part, 1, 1] = take(up(p, side - 1), 0)
            for way in range(2):
                r1_copy(part, s, part, way).start()

    def do_r2(s):
        c = lax.rem(s, ring)
        for part, way in both:
            r1_copy(part, s, part, way).wait_recv()
            p = place[part]
            q = up(p) if way == 0 else up(p, side - 1)
            s2[s, part, way] = (acc[c, at(q, block), lane(part, way)] + r1[s, part, way, 0].astype(F32)).astype(BF16)
            r2_copy(part, s, part, way).start()

    def do_r3(s):
        c = lax.rem(s, ring)
        for part in range(2):
            p, q = place[part], place[1 - part]
            for way in range(2):
                r2_copy(part, s, part, way).wait_recv()
                mid[c, part, way] = (acc[c, at(p, block), lane(part, way)] + r1[s, part, 1 - way, 1].astype(F32)
                                     + r2[s, part, way].astype(F32))

            def take(r, half):
                return mid[c, part, half, at(r, piece)].astype(BF16)

            s3[s, part, 0, 0] = take(up(q, 2), 0)
            s3[s, part, 0, 1] = take(up(q), 1)
            s3[s, part, 1, 0] = take(up(q, 2), 1)
            s3[s, part, 1, 1] = take(up(q, side - 1), 0)
            for way in range(2):
                r3_copy(1 - part, s, part, way).start()

    def do_r4(s):
        c = lax.rem(s, ring)
        for part, way in both:
            r3_copy(1 - part, s, part, way).wait_recv()
            q = place[1 - part]
            r = up(q) if way == 0 else up(q, side - 1)
            s4[s, part, way] = (mid[c, part, way, at(r, piece)] + r3[s, part, way, 0].astype(F32)).astype(BF16)
            r4_copy(1 - part, s, part, way).start()

    def do_g1(s):
        c = lax.rem(s, ring)
        for part in range(2):
            p, q = place[part], place[1 - part]
            for way in range(2):
                r4_copy(1 - part, s, part, way).wait_recv()
                total = (mid[c, part, way, at(q, piece)] + r3[s, part, 1 - way, 1].astype(F32)
                         + r4[s, part, way].astype(F32))
                ag[0, s, 2 * part + way, at(p * side + q, piece)] = total.astype(BF16)
            for way in range(2):
                g1_copy(s, part, way).start()

    def do_g2(s):
        for part, way in both:
            g1_copy(s, part, way).wait_recv()
            g2_copy(s, part, way).start()

    def do_g3(s):
        for part in range(2):
            for way in range(2):
                g2_copy(s, part, way).wait_recv()
            for way in range(2):
                g3_copy(s, part, way).start()

    def do_g4(s):
        for part, way in both:
            g3_copy(s, part, way).wait_recv()
            g4_copy(s, part, way).start()

    def do_z(s):
        for part, way in both:
            g4_copy(s, part, way).wait_recv()
        z_copy(s).start()
        for copy in out_copies(0, s):
            copy.start()

    def do_end(s):
        z_copy(s).wait_recv()
        for copy in out_copies(1, s):
            copy.start()

    later = [do_r2, do_r3, do_r4, do_g1, do_g2, do_g3, do_g4, do_z, do_end]

    def term(m, h, slot):
        return lax.dot_general(av[m, h], gv[m, slot], (((0,), (0,)), ((), ())), preferred_element_type=F32)

    def turn(i, carry):
        j, h = lax.div(i, splits), lax.rem(i, splits)
        slot = lax.rem(j, 2)
        computes = i < chunks

        @pl.when(computes)
        def _():
            @pl.when(h == 0)
            def _():
                @pl.when(i + splits < chunks)
                def _():
                    for m in range(2):
                        g_copy(m, j + 1, 1 - slot).start()

                g_copy(0, j, slot).wait()

            @pl.when(j == 0)
            def _():
                a_copy(0, h).wait()

            es[i] = term(0, h, slot).astype(BF16)
            e_copy(i).start()

        for n in reversed(range(len(later))):
            s = i - (n + 1)

            @pl.when((s >= 0) & (s < chunks))
            def _():
                later[n](s)

        @pl.when(computes)
        def _():
            @pl.when(h == 0)
            def _():
                g_copy(1, j, slot).wait()

            @pl.when(j == 0)
            def _():
                a_copy(1, h).wait()

            c = lax.rem(i, ring)
            acc[c] = term(1, h, slot)
            e_copy(i).wait_recv()
            acc[c] += er[i].astype(F32)
            start_r1(i)

        return carry

    lax.fori_loop(0, chunks + len(later), turn, 0)

    sent = [es, es, s1, s2, s3, s4, s3, s4, s1, s2]
    for stage, ref in enumerate(sent):
        pltpu.make_async_copy(ref, ref, send_sem.at[stage]).wait()
    pltpu.make_async_copy(ag, ag, o_sem).wait()


def solution(mesh):
    side = math.isqrt(mesh.shape["dp"] // 2)

    def step(a, g):
        _, matrices, tokens, d = a.shape
        ff = g.shape[3]
        assert matrices == 2 and side == 4
        splits = 2
        rows = d // splits
        chunks = splits * ff // COLS
        block, piece = rows // side, rows // side // side

        def halves(n, *shape):
            return pltpu.VMEM((chunks, 2, 2, *n, *shape, LANES), BF16)

        dma = pltpu.SemaphoreType.DMA
        return pl.pallas_call(
            functools.partial(kernel, side),
            out_shape=jax.ShapeDtypeStruct((matrices, d, ff), BF16),
            in_specs=[pl.BlockSpec(memory_space=pl.ANY)] * 2,
            out_specs=pl.BlockSpec(memory_space=pl.ANY),
            scratch_shapes=[
                pltpu.VMEM((2, splits, tokens, rows), BF16),
                pltpu.VMEM((2, 2, tokens, COLS), BF16),
                pltpu.VMEM((4, rows, COLS), F32),
                pltpu.VMEM((4, 2, 2, block, LANES), F32),
                pltpu.VMEM((chunks, rows, COLS), BF16),
                pltpu.VMEM((chunks, rows, COLS), BF16),
                halves((2,), block), halves((2,), block),
                halves((), block), halves((), block),
                halves((2,), piece), halves((2,), piece),
                halves((), piece), halves((), piece),
                pltpu.VMEM((2, chunks, COLS // LANES, rows, LANES), BF16),
                dma((2, splits)), dma((2, 2)), dma(()), dma((10,)),
                dma((chunks,)), *[dma((chunks, 2, 2))] * 8, dma((chunks,)),
            ],
            compiler_params=pltpu.CompilerParams(
                collective_id=0, has_side_effects=True, vmem_limit_bytes=63 * 2**20),
        )(a, g)

    return jax.shard_map(
        step, mesh=mesh, in_specs=(P(("rep", "dp")), P(("rep", "dp"))), out_specs=P("rep"), check_vma=False)
```

```python
import functools
import math

import jax
import jax.numpy as jnp
from jax import lax
from jax.experimental import pallas as pl
from jax.experimental.pallas import tpu as pltpu
from jax.sharding import PartitionSpec as P

MESH = pl.DeviceIdType.MESH
F32, BF16 = jnp.float32, jnp.bfloat16
COLS = 512
VMEM_LIMIT = 54
LAGS = (1, 3, 5, 7, 9, 10)


def sum_kernel(side, a_ref, g_ref, ag, av, gv, acc, mid, es, er, s1, r1, s2, r2,
               a_sem, g_sem, send_sem, e_r, r1_r, r2_r, g2_r, g1_r, z_r):
    chunks, rows = es.shape[0], es.shape[1]
    splits = av.shape[1]
    block, piece = rows // side, rows // side // side
    ring, ring_mid = acc.shape[0], mid.shape[0]

    me = lax.axis_index("dp")
    core = lax.rem(me, 2)
    y = lax.rem(lax.div(me, 2), side)
    x = lax.div(me, 2 * side)

    def device(x, y, core):
        return (x * side + y) * 2 + core

    def up(p, by):
        return lax.rem(p + by, side)

    steps = tuple(range(1, side))
    far_first = sorted(steps, key=lambda k: -min(k, side - k))
    peer = device(x, y, 1 - core)
    on_x = [device(up(x, k), y, core) for k in steps]
    on_y = [device(x, up(y, k), core) for k in steps]

    def axes(s):
        odd = lax.rem(s, 2)

        def pick(u, v):
            return jnp.where(odd == 0, u, v)

        return (pick(x, y), pick(y, x), [pick(u, v) for u, v in zip(on_x, on_y)],
                [pick(v, u) for u, v in zip(on_x, on_y)])

    def a_copy(m, h):
        matrix = 1 - core if m == 0 else core
        return pltpu.make_async_copy(a_ref.at[0, matrix, :, pl.ds(h * rows, rows)], av.at[m, h], a_sem.at[m, h])

    def g_copy(m, j, slot):
        matrix = 1 - core if m == 0 else core
        columns = pl.ds(pl.multiple_of(j * COLS, COLS), COLS)
        return pltpu.make_async_copy(g_ref.at[0, matrix, :, columns], gv.at[m, slot], g_sem.at[m, slot])

    for m in range(2):
        a_copy(m, 0).start()
        g_copy(m, 0, 0).start()
    for m in range(2):
        for h in range(1, splits):
            a_copy(m, h).start()

    barrier = pltpu.get_barrier_semaphore()
    partners = (peer, *on_x, *on_y)
    for partner in partners:
        pl.semaphore_signal(barrier, inc=1, device_id={"dp": partner}, device_id_type=MESH)

    def remote(src, dst, stage, recv, to):
        return pltpu.make_async_remote_copy(
            src_ref=src, dst_ref=dst, send_sem=send_sem.at[stage], recv_sem=recv, device_id={"dp": to},
            device_id_type=MESH)

    def at(p, size):
        return pl.ds(pl.multiple_of(p * size, size), size)

    def e_copy(s):
        return remote(es.at[s], er.at[s], 0, e_r.at[s], peer)

    def r1_copy(s, k, to):
        return remote(s1.at[s, k - 1], r1.at[s, k - 1], 1, r1_r.at[s, k - 1], to)

    def r2_copy(s, k, to):
        return remote(s2.at[s, k - 1], r2.at[s, k - 1], 2, r2_r.at[s, k - 1], to)

    def g2_copy(s, k, to, p, q):
        view = ag.at[0, s, at(p * side + q, piece)]
        return remote(view, view, 3, g2_r.at[s, k - 1], to)

    def g1_copy(s, k, to, p):
        view = ag.at[0, s, at(p, block)]
        return remote(view, view, 4, g1_r.at[s, k - 1], to)

    def z_copy(s):
        return remote(ag.at[0, s], ag.at[1, s], 5, z_r.at[s], peer)

    def do_e(s):
        c = lax.rem(s, ring)
        p, _, first, _ = axes(s)
        e_copy(s).wait_recv()
        acc[c] += er[s].astype(F32)
        for k in far_first:
            s1[s, k - 1] = acc[c, at(up(p, k), block)].astype(BF16)
            r1_copy(s, k, first[k - 1]).start()

    def do_r2(s):
        c, d = lax.rem(s, ring), lax.rem(s, ring_mid)
        p, q, first, second = axes(s)
        for k in steps:
            r1_copy(s, k, first[k - 1]).wait_recv()
        total = acc[c, at(p, block)]
        for k in steps:
            total += r1[s, k - 1].astype(F32)
        mid[d] = total
        for k in far_first:
            s2[s, k - 1] = mid[d, at(up(q, k), piece)].astype(BF16)
            r2_copy(s, k, second[k - 1]).start()

    def do_g2(s):
        d = lax.rem(s, ring_mid)
        p, q, _, second = axes(s)
        for k in steps:
            r2_copy(s, k, second[k - 1]).wait_recv()
        total = mid[d, at(q, piece)]
        for k in steps:
            total += r2[s, k - 1].astype(F32)
        ag[0, s, at(p * side + q, piece)] = total.astype(BF16)
        for k in far_first:
            g2_copy(s, k, second[k - 1], p, q).start()

    def do_g1(s):
        p, q, first, second = axes(s)
        for k in steps:
            g2_copy(s, k, second[k - 1], p, q).wait_recv()
        for k in far_first:
            g1_copy(s, k, first[k - 1], p).start()

    def do_z(s):
        p, _, first, _ = axes(s)
        for k in steps:
            g1_copy(s, k, first[k - 1], p).wait_recv()
        z_copy(s).start()

    def do_end(s):
        z_copy(s).wait_recv()

    later = (do_e, do_r2, do_g2, do_g1, do_z, do_end)

    def term(m, h, slot):
        return lax.dot_general(av[m, h], gv[m, slot], (((0,), (0,)), ((), ())), preferred_element_type=F32)

    def turn(i, carry):
        j, h = lax.div(i, splits), lax.rem(i, splits)
        slot = lax.rem(j, 2)
        computes = i < chunks

        @pl.when(computes)
        def _():
            @pl.when(h == 0)
            def _():
                @pl.when(i + splits < chunks)
                def _():
                    for m in range(2):
                        g_copy(m, j + 1, 1 - slot).start()

                g_copy(0, j, slot).wait()

            @pl.when(j == 0)
            def _():
                a_copy(0, h).wait()

            es[i] = term(0, h, slot).astype(BF16)

            @pl.when(i == 0)
            def _():
                pl.semaphore_wait(barrier, len(partners))

            e_copy(i).start()

        for lag, step in zip(LAGS, later):
            s = i - lag

            @pl.when((s >= 0) & (s < chunks))
            def _():
                step(s)

        @pl.when(computes)
        def _():
            @pl.when(h == 0)
            def _():
                g_copy(1, j, slot).wait()

            @pl.when(j == 0)
            def _():
                a_copy(1, h).wait()

            acc[lax.rem(i, ring)] = term(1, h, slot)

        return carry

    lax.fori_loop(0, chunks + LAGS[-1], turn, 0)

    sent = [es, s1, s2, s2, s1, es]
    for stage, ref in enumerate(sent):
        pltpu.make_async_copy(ref, ref, send_sem.at[stage]).wait()


def out_kernel(splits, v_ref, out_ref, sem):
    _, chunks, rows, columns = v_ref.shape
    core = lax.rem(lax.axis_index("dp"), 2)
    copies = []
    for m in range(2):
        for s in range(chunks):
            j, h = s // splits, s % splits
            copies.append(pltpu.make_async_copy(
                v_ref.at[m, s],
                out_ref.at[core if m == 0 else 1 - core, pl.ds(h * rows, rows), pl.ds(j * columns, columns)],
                sem.at[m, s]))
    for copy in copies:
        copy.start()
    for copy in copies:
        copy.wait()


def solution(mesh):
    side = math.isqrt(mesh.shape["dp"] // 2)

    def step(a, g):
        _, matrices, tokens, d = a.shape
        ff = g.shape[3]
        assert matrices == 2
        splits = 2
        rows = d // splits
        chunks = splits * ff // COLS
        block, piece = rows // side, rows // side // side
        others = side - 1
        ring = LAGS[1] + 1
        ring_mid = LAGS[2] - LAGS[1] + 1
        dma = pltpu.SemaphoreType.DMA
        gathered = pl.pallas_call(
            functools.partial(sum_kernel, side),
            out_shape=pltpu.VMEM((matrices, chunks, rows, COLS), BF16),
            in_specs=[pl.BlockSpec(memory_space=pl.ANY)] * 2,
            out_specs=pl.BlockSpec(memory_space=pltpu.VMEM),
            scratch_shapes=[
                pltpu.VMEM((2, splits, tokens, rows), BF16),
                pltpu.VMEM((2, 2, tokens, COLS), BF16),
                pltpu.VMEM((ring, rows, COLS), F32),
                pltpu.VMEM((ring_mid, block, COLS), F32),
                pltpu.VMEM((chunks, rows, COLS), BF16),
                pltpu.VMEM((chunks, rows, COLS), BF16),
                pltpu.VMEM((chunks, others, block, COLS), BF16),
                pltpu.VMEM((chunks, others, block, COLS), BF16),
                pltpu.VMEM((chunks, others, piece, COLS), BF16),
                pltpu.VMEM((chunks, others, piece, COLS), BF16),
                dma((2, splits)), dma((2, 2)), dma((6,)),
                dma((chunks,)), *[dma((chunks, others))] * 4, dma((chunks,)),
            ],
            compiler_params=pltpu.CompilerParams(
                collective_id=0, has_side_effects=True, vmem_limit_bytes=VMEM_LIMIT * 2**20),
        )(a, g)
        return pl.pallas_call(
            functools.partial(out_kernel, splits),
            out_shape=jax.ShapeDtypeStruct((matrices, d, ff), BF16),
            in_specs=[pl.BlockSpec(memory_space=pltpu.VMEM)],
            out_specs=pl.BlockSpec(memory_space=pl.ANY),
            scratch_shapes=[dma((matrices, chunks))],
            compiler_params=pltpu.CompilerParams(vmem_limit_bytes=2**20),
        )(gathered)

    return jax.shard_map(
        step, mesh=mesh, in_specs=(P(("rep", "dp")), P(("rep", "dp"))), out_specs=P("rep"), check_vma=False)
```

```python
import functools
import math

import jax
import jax.numpy as jnp
from jax import lax
from jax.experimental import pallas as pl
from jax.experimental.pallas import tpu as pltpu
from jax.sharding import PartitionSpec as P

MESH = pl.DeviceIdType.MESH
F32, BF16 = jnp.float32, jnp.bfloat16
COLS = 512
HALF = COLS // 2
VMEM_LIMIT = 54
LAST = 2
RING = (("r2", 5, 4.8), ("g2", 8, 3.6), ("g1", 11, 3.6), ("g1_next", 15, 4.0), ("z", 22, 3.5), ("end", 24, 1.3))
LONG = (("r2", 4, 4.8), ("g2", 7, 3.6), ("g1", 10, 3.6), ("z", 14, 4.8), ("end", 16, 1.3))
TURN = 3.15


def last_steps(chunks):
    ready = []
    for s in range(chunks):
        kind = kind_of(s, chunks)
        before = (s + 1 - chunks) * TURN
        for n, (name, lag, hop) in enumerate(kind):
            if s + (lag + 1) // 2 < chunks:
                before = (s + 1 - chunks) * TURN + lag * TURN / 2
            else:
                ready.append((before + hop, n, s, name))
                before = max(before + hop, 0.0)
    return [(s, name) for _, _, s, name in sorted(ready)]


def kind_of(s, chunks):
    return RING if s < chunks - LAST else LONG


def sum_kernel(side, a_ref, g_ref, ag, av, gv, acc, mid, es, er, s1, r1, s2, r2,
               a_sem, g_sem, send_sem, e_r, r1_r, r2_r, g2_r, g1_r, m1_r, z_r):
    chunks, rows = es.shape[0], es.shape[1]
    splits = av.shape[1]
    block, piece = rows // side, rows // side // side
    ring, ring_mid = acc.shape[0], mid.shape[0]

    me = lax.axis_index("dp")
    core = lax.rem(me, 2)
    y = lax.rem(lax.div(me, 2), side)
    x = lax.div(me, 2 * side)

    def device(x, y, core):
        return (x * side + y) * 2 + core

    def up(p, by):
        return lax.rem(p + by, side)

    steps = tuple(range(1, side))
    far_first = sorted(steps, key=lambda k: -min(k, side - k))
    peer = device(x, y, 1 - core)
    on_x = [device(up(x, k), y, core) for k in steps]
    on_y = [device(x, up(y, k), core) for k in steps]

    def rem(s, n):
        return s % n if isinstance(s, int) else lax.rem(s, n)

    def axes(s):
        odd = rem(s, 2)

        def pick(u, v):
            return (v if odd else u) if isinstance(s, int) else jnp.where(odd == 0, u, v)

        return (pick(x, y), pick(y, x), [pick(u, v) for u, v in zip(on_x, on_y)],
                [pick(v, u) for u, v in zip(on_x, on_y)])

    def a_copy(m, h):
        matrix = 1 - core if m == 0 else core
        return pltpu.make_async_copy(a_ref.at[0, matrix, :, pl.ds(h * rows, rows)], av.at[m, h], a_sem.at[m, h])

    def g_copy(m, j, slot):
        matrix = 1 - core if m == 0 else core
        columns = pl.ds(pl.multiple_of(j * COLS, COLS), COLS)
        return pltpu.make_async_copy(g_ref.at[0, matrix, :, columns], gv.at[m, slot], g_sem.at[m, slot])

    a_copy(0, 0).start()
    g_copy(0, 0, 0).start()

    barrier = pltpu.get_barrier_semaphore()
    partners = (peer, *on_x, *on_y)
    for partner in partners:
        pl.semaphore_signal(barrier, inc=1, device_id={"dp": partner}, device_id_type=MESH)

    def remote(src, dst, stage, recv, to):
        return pltpu.make_async_remote_copy(
            src_ref=src, dst_ref=dst, send_sem=send_sem.at[stage], recv_sem=recv, device_id={"dp": to},
            device_id_type=MESH)

    def at(p, size):
        return pl.ds(pl.multiple_of(p * size, size), size)

    def e_copy(s):
        return remote(es.at[s], er.at[s], 0, e_r.at[s], peer)

    def z_copy(s):
        return remote(ag.at[0, s], ag.at[1, s], 5, z_r.at[s], peer)

    def r1_copy(s, k, to):
        part = pl.ds(2 * (k - 1), 2)
        return remote(s1.at[s, part], r1.at[s, part], 1, r1_r.at[s], to)

    def r2_copy(s, k, to):
        return remote(s2.at[s, k - 1], r2.at[s, k - 1], 2, r2_r.at[s], to)

    def g2_copy(s, k, to, p, q):
        view = ag.at[0, s, at(p * side + q, piece)]
        return remote(view, view, 3, g2_r.at[s], to)

    def g1_copy(s, to, p):
        view = ag.at[0, s, at(p, block)]
        return remote(view, view, 4, g1_r.at[s], to)

    def g1_next(s, way, to, p):
        view = ag.at[0, s, at(p, block), pl.ds(way * HALF, HALF)]
        return remote(view, view, 4, m1_r.at[s], to)

    def landed(ref, sem):
        pltpu.make_async_copy(ref, ref, sem).wait()

    def half(h):
        return slice(h * HALF, (h + 1) * HALF)

    def ends(first):
        return first[0], first[-1]

    def start_r1(s):
        c = rem(s, ring)
        p, _, first, _ = axes(s)
        for k in far_first:
            for h in range(2):
                s1[s, 2 * (k - 1) + h] = acc[c, at(up(p, k), block), half(h)].astype(BF16)
            r1_copy(s, k, first[k - 1]).start()

    def do_r2(s, straight):
        c, d = rem(s, ring), rem(s, ring_mid)
        p, q, _, second = axes(s)
        landed(r1.at[s], r1_r.at[s])
        for h in range(2):
            total = acc[c, at(p, block), half(h)]
            for k in steps:
                total += r1[s, 2 * (k - 1) + h].astype(F32)
            mid[d, :, half(h)] = total
        for k in far_first:
            s2[s, k - 1] = mid[d, at(up(q, k), piece)].astype(BF16)
            r2_copy(s, k, second[k - 1]).start()

    def do_g2(s, straight):
        d = rem(s, ring_mid)
        p, q, _, second = axes(s)
        landed(r2.at[s], r2_r.at[s])
        total = mid[d, at(q, piece)]
        for k in steps:
            total += r2[s, k - 1].astype(F32)
        ag[0, s, at(p * side + q, piece)] = total.astype(BF16)
        for k in far_first:
            g2_copy(s, k, second[k - 1], p, q).start()

    def do_g1(s, straight):
        p, q, first, second = axes(s)
        landed(r2.at[s], g2_r.at[s])
        if straight:
            for k in far_first:
                g1_copy(s, first[k - 1], p).start()
        else:
            for way, to in enumerate(ends(first)):
                g1_copy(s, to, p).start()

    def do_g1_next(s, straight):
        p, _, first, _ = axes(s)
        landed(r1.at[s, 0:4], g1_r.at[s])
        for way, to in enumerate(ends(first)):
            g1_next(s, way, to, up(p, side - 1 if way == 0 else 1)).start()

    def do_z(s, straight):
        p, _, first, _ = axes(s)
        if straight:
            landed(r1.at[s], g1_r.at[s])
        else:
            landed(r1.at[s, 4:6], m1_r.at[s])
        z_copy(s).start()

    def do_end(s, straight):
        z_copy(s).wait_recv()

    steps_of = dict(r2=do_r2, g2=do_g2, g1=do_g1, g1_next=do_g1_next, z=do_z, end=do_end)
    kinds = ((RING, 0, chunks - LAST), (LONG, chunks - LAST, chunks))

    def term(m, h, slot):
        return lax.dot_general(av[m, h], gv[m, slot], (((0,), (0,)), ((), ())), preferred_element_type=F32)

    def due(i, odd):
        for kind, low, high in kinds:
            for name, lag, _ in kind:
                turns = (lag + 1) // 2
                if lag % 2 == odd and low < high and low + turns < chunks:

                    @pl.when((i - turns >= low) & (i - turns < high))
                    def _():
                        steps_of[name](i - turns, kind is LONG)

    def turn(i, carry):
        n = i + 1
        j, h = lax.div(n, splits), lax.rem(n, splits)
        slot = lax.rem(j, 2)

        @pl.when(n < chunks)
        def _():
            @pl.when(h == 0)
            def _():
                @pl.when((n > 0) & (n + splits < chunks))
                def _():
                    g_copy(0, j + 1, 1 - slot).start()

                g_copy(0, j, slot).wait()

            @pl.when(j == 0)
            def _():
                a_copy(0, h).wait()

            @pl.when(n == 0)
            def _():
                for h in range(1, splits):
                    a_copy(0, h).start()
                a_copy(1, 0).start()
                g_copy(1, 0, 0).start()
                for h in range(1, splits):
                    a_copy(1, h).start()
                g_copy(0, 1, 1).start()

            es[n] = term(0, h, slot).astype(BF16)

            @pl.when(n == 0)
            def _():
                pl.semaphore_wait(barrier, len(partners))

            e_copy(n).start()

        due(i, 1)

        @pl.when(i >= 0)
        def _():
            j, h = lax.div(i, splits), lax.rem(i, splits)
            slot = lax.rem(j, 2)

            @pl.when(h == 0)
            def _():
                @pl.when(i + splits < chunks)
                def _():
                    g_copy(1, j + 1, 1 - slot).start()

                g_copy(1, j, slot).wait()

            @pl.when(j == 0)
            def _():
                a_copy(1, h).wait()

            e_copy(i).wait_recv()
            acc[lax.rem(i, ring)] = term(1, h, slot) + er[i].astype(F32)
            start_r1(i)

        due(i, 0)
        return carry

    lax.fori_loop(-1, chunks, turn, 0)
    for s, name in last_steps(chunks):
        steps_of[name](s, kind_of(s, chunks) is LONG)

    sent = [es, s1, s2, s2, s1, es]
    for stage, ref in enumerate(sent):
        pltpu.make_async_copy(ref, ref, send_sem.at[stage]).wait()


def out_kernel(splits, v_ref, out_ref, sem):
    _, chunks, rows, columns = v_ref.shape
    core = lax.rem(lax.axis_index("dp"), 2)
    copies = []
    for m in range(2):
        for s in range(chunks):
            j, h = s // splits, s % splits
            copies.append(pltpu.make_async_copy(
                v_ref.at[m, s],
                out_ref.at[core if m == 0 else 1 - core, pl.ds(h * rows, rows), pl.ds(j * columns, columns)],
                sem.at[m, s]))
    for copy in copies:
        copy.start()
    for copy in copies:
        copy.wait()


def solution(mesh):
    side = math.isqrt(mesh.shape["dp"] // 2)

    def step(a, g):
        _, matrices, tokens, d = a.shape
        ff = g.shape[3]
        assert matrices == 2 and side == 4
        splits = 2
        rows = d // splits
        chunks = splits * ff // COLS
        block, piece = rows // side, rows // side // side
        others = side - 1
        ring = 8
        ring_mid = 8
        dma = pltpu.SemaphoreType.DMA
        gathered = pl.pallas_call(
            functools.partial(sum_kernel, side),
            out_shape=pltpu.VMEM((matrices, chunks, rows, COLS), BF16),
            in_specs=[pl.BlockSpec(memory_space=pl.ANY)] * 2,
            out_specs=pl.BlockSpec(memory_space=pltpu.VMEM),
            scratch_shapes=[
                pltpu.VMEM((2, splits, tokens, rows), BF16),
                pltpu.VMEM((2, 2, tokens, COLS), BF16),
                pltpu.VMEM((ring, rows, COLS), F32),
                pltpu.VMEM((ring_mid, block, COLS), F32),
                pltpu.VMEM((chunks, rows, COLS), BF16),
                pltpu.VMEM((chunks, rows, COLS), BF16),
                pltpu.VMEM((chunks, 6, block, HALF), BF16),
                pltpu.VMEM((chunks, 6, block, HALF), BF16),
                pltpu.VMEM((chunks, others, piece, COLS), BF16),
                pltpu.VMEM((chunks, others, piece, COLS), BF16),
                dma((2, splits)), dma((2, 2)), dma((6,)),
                *[dma((chunks,))] * 7,
            ],
            compiler_params=pltpu.CompilerParams(
                collective_id=0, has_side_effects=True, vmem_limit_bytes=VMEM_LIMIT * 2**20),
        )(a, g)
        return pl.pallas_call(
            functools.partial(out_kernel, splits),
            out_shape=jax.ShapeDtypeStruct((matrices, d, ff), BF16),
            in_specs=[pl.BlockSpec(memory_space=pltpu.VMEM)],
            out_specs=pl.BlockSpec(memory_space=pl.ANY),
            scratch_shapes=[dma((matrices, chunks))],
            compiler_params=pltpu.CompilerParams(vmem_limit_bytes=2**20),
        )(gathered)

    return jax.shard_map(
        step, mesh=mesh, in_specs=(P(("rep", "dp")), P(("rep", "dp"))), out_specs=P("rep"), check_vma=False)
```
